32 devices in a mesh: member: 2 (over y), tile: 8 (over z, x), sub: 2 (over core).
Axes of the slice: x: 2, y: 2, z: 4, core: 2. Of those that a mesh axis runs over, the one named last changes fastest.
Arguments:
- atm_state: bfloat16 [8, 32768], P(None, ('member', 'tile')), parts along dimension 1, may hold values from -6 to 6
- ocn_state: bfloat16 [4, 32768], P(None, ('member', 'tile', 'sub')), parts along dimension 1, may hold values from -6 to 6
- need_atm: int32 [128], P(('tile', 'sub')), may hold values from 0 to 127, as said below
- xb_need: int32 [128], P(('tile', 'sub')), may hold values from 0 to 15
- xb_ocn: int32 [128], P(('tile', 'sub')), may hold values from 0 to 15
- xb_count: int32 [16], P(('tile', 'sub')), may hold values from 1 to 8, as said below
- sea_mask: int32 [16384], P(('tile', 'sub')), may hold values 0 or 1
- cell_area: float32 [16384], P(('tile', 'sub')), may hold values from 0.5 to 2
- w_atm: bfloat16 [128, 128, 128], P(('tile', 'sub')), may hold values from 0.0099487305 to 1
- w_ocn: bfloat16 [128, 128, 128], P(('tile', 'sub')), may hold values from 0.0099487305 to 1
Outputs:
- atm_flux: float32 [4, 32768], P(None, ('member', 'tile')), parts along dimension 1
- ocn_flux: float32 [4, 32768], P(None, ('member', 'tile', 'sub')), parts along dimension 1
The draws below stay inside these ranges and needn't reach their ends.
There are 2 independent parts, one for each index of `member`. The reference program is written for one: setup_inputs(seed, part) draws one part's arguments, and reference() takes and returns one part's arrays. A program takes and returns all parts, laid end to end along the dimension named above; an argument that names none is the same for every part. Nothing has to cross between parts.
Inputs may be any that keep to these rules, and one draw needn't show every extreme that they name: `need_atm`: an atmosphere block n lies on tile n // 16. A tile's list is the entries of its devices in device order; for tile t its entries 2 i and 2 i + 1 lie on tile (t + i - 8 // 2 + 1) mod 8 for i < 7, and on tile (t + 4) mod 8 for i = 7; all entries of one tile's list are distinct. `xb_need`: index into the list of the block's tile. `xb_ocn`: index among the ocean blocks of the block's tile, in device order. `xb_count`: some device has all 8 blocks live.
All inputs are finite; a program needn't handle non-finite values. No bound on the sum of `sea_mask` on one device may be relied on, other than what follows from the above.
Results may differ from the reference program's by a relative error of at most 0.0003.
Values may be sent and summed in bfloat16 or wider, within the bound.
No kernel may reach another device: no remote copies, remote signals or barrier semaphores. Data moves between devices by JAX's collectives and lax.ppermute only.
A program may use at most 64 MiB of HBM per device.

```python
import math
import jax
import jax.numpy as jnp
from jax import lax

F_A = 8
F_O = 4
F_X = 4
BLK = 128
ABLK_TILE = 16
OBLK_DEV = 8
XB_DEV = 8
NEED_DEV = 8
ATM_CELLS = 16384
OCN_CELLS = 16384
XBLKS = 128
N_TILE = 8
N_SUB = 2


def draw_need_atm(key, part):
    first, second = jax.random.split(key, 2)
    lower = jax.random.randint(first, (N_TILE, NEED_DEV), 0, ABLK_TILE)
    apart = jax.random.randint(second, (N_TILE, NEED_DEV), 1, ABLK_TILE)
    upper = (lower + apart) % ABLK_TILE
    locals_pair = jnp.stack([lower, upper], 2)
    order = jnp.arange(NEED_DEV, dtype=jnp.int32)
    offset = jnp.where(order < NEED_DEV - 1, order - NEED_DEV // 2 + 1, N_TILE // 2)
    owner = (jnp.arange(N_TILE, dtype=jnp.int32)[:, None] + offset[None, :]) % N_TILE
    return (owner[:, :, None] * ABLK_TILE + locals_pair).reshape(-1).astype(jnp.int32)


def draw_xb_count(key, part):
    devices = N_TILE * N_SUB
    shifts = jax.random.randint(key, (devices,), 0, 3)
    chosen = jax.random.randint(jax.random.fold_in(key, 7), (), 0, devices)
    shifts = jnp.where(jnp.arange(devices) == chosen, 0, shifts)
    return (XB_DEV // jnp.left_shift(1, shifts)).astype(jnp.int32)


def with_ends(array, own_key, least, largest):
    dims = array.shape
    place = [jax.random.randint(jax.random.fold_in(own_key, axis), (), 0, dims[axis]) for axis in range(len(dims))]
    array = array.at[tuple(place)].set(least)
    longest = dims.index(max(dims))
    place[longest] = (place[longest] + 1) % dims[longest]
    return array.at[tuple(place)].set(largest)


def block_scale(key, extent, cuts, smallest, top_value):
    level = 1.0
    for position, shards_of in cuts:
        steps = jax.random.uniform(jax.random.fold_in(jax.random.fold_in(key, 6), position), (shards_of,), jnp.float32, smallest / len(cuts), top_value / len(cuts))
        level = level * jnp.repeat(jnp.exp(steps), extent[position] // shards_of).reshape((-1,) + (1,) * (len(extent) - 1 - position))
    return level


def scatter_about(rng, dims, spread, limit, cuts=(), kind=jnp.bfloat16):
    level = block_scale(rng, dims, cuts, -0.22, 0.18) if cuts else 1.0
    entries = jax.random.normal(rng, dims, jnp.float32) * spread * level
    return jnp.minimum(jnp.maximum(entries, -limit), limit).astype(kind)


def setup_inputs(seed: int = 0, part: int = 0) -> dict:
    key_list = jax.random.split(jax.random.key(seed), 11)
    own_keys = jax.random.split(jax.random.fold_in(key_list[10], part), 11)
    return {
        "atm_state": scatter_about(own_keys[0], (F_A, ATM_CELLS), 1.0, 6.0, ((1, 8),)),
        "ocn_state": scatter_about(own_keys[1], (F_O, OCN_CELLS), 1.0, 6.0, ((1, 16),)),
        "need_atm": draw_need_atm(jax.random.fold_in(key_list[10], 71), part),
        "xb_need": with_ends(jax.random.randint(key_list[3], (XBLKS,), 0, N_SUB * NEED_DEV), jax.random.fold_in(key_list[3], 1), 0, (N_SUB * NEED_DEV) - 1).astype(jnp.int32),
        "xb_ocn": with_ends(jax.random.randint(key_list[4], (XBLKS,), 0, N_SUB * OBLK_DEV), jax.random.fold_in(key_list[4], 1), 0, (N_SUB * OBLK_DEV) - 1).astype(jnp.int32),
        "xb_count": draw_xb_count(jax.random.fold_in(key_list[10], 71), part),
        "sea_mask": with_ends((jax.random.randint(key_list[6], (XBLKS * BLK,), 0, 3) < 2).astype(jnp.int32), jax.random.fold_in(key_list[6], 1), 0, 1),
        "cell_area": jnp.clip(jnp.exp(math.log(2.0) - 1.3862944 * jax.random.uniform(key_list[7], (XBLKS * BLK,), jnp.float32) ** block_scale(key_list[7], (XBLKS * BLK,), ((0, 16),), -0.2, 0.2)), 0.5, 2.0),
        "w_atm": jnp.clip(jnp.exp(math.log(1.0) - 4.61031033 * jax.random.uniform(key_list[8], (XBLKS, BLK, BLK), jnp.float32) ** block_scale(key_list[8], (XBLKS, BLK, BLK), ((0, 16),), -0.2, 0.2)), 0.0099487305, 1.0).astype(jnp.bfloat16),
        "w_ocn": jnp.clip(jnp.exp(math.log(1.0) - 4.61031033 * jax.random.uniform(key_list[9], (XBLKS, BLK, BLK), jnp.float32) ** block_scale(key_list[9], (XBLKS, BLK, BLK), ((0, 16),), -0.2, 0.2)), 0.0099487305, 1.0).astype(jnp.bfloat16),
    }


def bulk_fluxes(upper_domain_vector, marine_regrid_transfer):
    lowest_level_warmth, vapour_mixing_ratio, eastward_wind, northward_wind, ground_level_pressure, solar_radiation, infrared_radiation, rainfall_rate = [upper_domain_vector[:, grid_box_number] for grid_box_number in range(8)]
    skin_warmth_kelvin, eastward_current, northward_current, marine_climate_coupler = [marine_regrid_transfer[:, grid_box_number] for grid_box_number in range(4)]
    du = eastward_wind - eastward_current
    dv = northward_wind - northward_current
    speed = jnp.sqrt(du * du + dv * dv + 1.0)
    momentum_transfer_factor = (0.3 + 0.1 * jnp.tanh(ground_level_pressure)) * speed
    conductive_energy_loss = momentum_transfer_factor * (skin_warmth_kelvin - lowest_level_warmth)
    evaporative_energy_loss = momentum_transfer_factor * (0.5 * skin_warmth_kelvin - vapour_mixing_ratio)
    taux = momentum_transfer_factor * du
    tauy = momentum_transfer_factor * dv
    reflected_fraction = 0.06 + 0.1 * jax.nn.sigmoid(marine_climate_coupler)
    thermal_energy_transfer = (1.0 - reflected_fraction) * solar_radiation + infrared_radiation - 0.2 * skin_warmth_kelvin - conductive_energy_loss - evaporative_energy_loss
    fresh = rainfall_rate - 0.5 * evaporative_energy_loss
    return (jnp.stack([conductive_energy_loss, evaporative_energy_loss, taux, tauy], 1), jnp.stack([thermal_energy_transfer, taux, tauy, fresh], 1))

def reference(atm_state, ocn_state, need_atm, xb_need, xb_ocn, xb_count, sea_mask, cell_area, w_atm, w_ocn):
    devices = N_TILE * N_SUB
    highest = lax.Precision.HIGHEST
    atm_table = jnp.transpose(atm_state.reshape(F_A, N_TILE * ABLK_TILE, BLK), (1, 0, 2))
    ocn_table = jnp.transpose(ocn_state.reshape(F_O, devices * OBLK_DEV, BLK), (1, 0, 2))
    list_len = N_SUB * NEED_DEV
    items = (jnp.arange(devices, dtype=jnp.int32), xb_need.reshape(devices, XB_DEV), xb_ocn.reshape(devices, XB_DEV), xb_count, sea_mask.reshape(devices, XB_DEV, BLK), cell_area.reshape(devices, XB_DEV, BLK), w_atm.reshape(devices, XB_DEV, BLK, BLK), w_ocn.reshape(devices, XB_DEV, BLK, BLK))

    def step(carry, item):
        acc_atm, acc_ocn = carry
        device, need_idx, ocn_idx, count, sea, area, weight_a, weight_o = item
        tile = device // N_SUB
        tile_list = lax.dynamic_slice_in_dim(need_atm, (tile * list_len).astype(jnp.int32), list_len)
        ids = tile_list[need_idx]
        oids = (tile * (N_SUB * OBLK_DEV) + ocn_idx).astype(jnp.int32)
        wa = weight_a.astype(jnp.float32)
        wo = weight_o.astype(jnp.float32)
        upper_domain_vector = jnp.einsum('bfj,bxj->bfx', atm_table[ids].astype(jnp.float32), wa, precision=highest) / lax.optimization_barrier(jnp.sum(wa, 2))[:, None, :]
        marine_regrid_transfer = jnp.einsum('bfj,bxj->bfx', ocn_table[oids].astype(jnp.float32), wo, precision=highest) / lax.optimization_barrier(jnp.sum(wo, 2))[:, None, :]
        to_atm, to_ocn = bulk_fluxes(upper_domain_vector, marine_regrid_transfer)
        live = (jnp.arange(XB_DEV, dtype=jnp.int32) < count).astype(jnp.float32)[:, None]
        weighted = area * live
        wet = weighted * sea.astype(jnp.float32)
        atm_terms = jnp.concatenate([to_atm * wet[:, None, :], weighted[:, None, :]], 1)
        ocn_terms = jnp.concatenate([to_ocn * wet[:, None, :], wet[:, None, :]], 1)
        atm_cells = jnp.einsum('bgx,bxj->bgj', atm_terms, wa, precision=highest)
        ocn_cells = jnp.einsum('bgx,bxj->bgj', ocn_terms, wo, precision=highest)
        return ((acc_atm.at[ids].add(atm_cells), acc_ocn.at[oids].add(ocn_cells)), None)
    init = (jnp.zeros((N_TILE * ABLK_TILE, F_X + 1, BLK), jnp.float32), jnp.zeros((devices * OBLK_DEV, F_X + 1, BLK), jnp.float32))
    (acc_atm, acc_ocn), _ = lax.scan(step, init, items)
    atm_flux = acc_atm[:, :F_X] / jnp.maximum(acc_atm[:, F_X:], 1.0)
    ocn_flux = acc_ocn[:, :F_X] / jnp.maximum(acc_ocn[:, F_X:], 1.0)
    atm_flux = jnp.transpose(atm_flux, (1, 0, 2)).reshape(F_X, N_TILE * ABLK_TILE * BLK)
    ocn_flux = jnp.transpose(ocn_flux, (1, 0, 2)).reshape(F_X, devices * OBLK_DEV * BLK)
    return (atm_flux, ocn_flux)
```

```python
import jax
import jax.numpy as jnp
from jax import lax
from jax.experimental import pallas as pl
from jax.experimental.pallas import tpu as pltpu
from jax.sharding import PartitionSpec as P

ROWS = 8
VM = pl.BlockSpec(memory_space=pltpu.VMEM)
SM = pl.BlockSpec(memory_space=pltpu.SMEM)


def split3(x):
    hi = x.astype(jnp.bfloat16)
    rest = x - hi.astype(jnp.float32)
    mid = rest.astype(jnp.bfloat16)
    lo = (rest - mid.astype(jnp.float32)).astype(jnp.bfloat16)
    return jnp.concatenate([hi, mid, lo], 0)


def select_kernel(npair, owned, blk):
    def body(pos, need, *refs):
        states, home, out = refs[: npair - 1], refs[npair - 1], refs[npair + 1]
        last = refs[npair]
        for j in range(npair):
            for e in range(2):
                n = need[2 * j + e] % owned
                at = pl.ds(pl.multiple_of(n * blk, blk), blk)
                if j < npair - 1:
                    out[2 * j + e] = states[j][:, at]
                else:

                    @pl.when(pos[1] == 0)
                    def _():
                        out[2 * j + e] = home[:, at]

                    @pl.when(pos[1] != 0)
                    def _():
                        out[2 * j + e] = last[:, at]

    return body


def main_kernel(nblocks, owned, blk, f_a, f_o, shifts, ntile, nsub):
    def body(
        pos, need, need2, xb_need, xb_ocn, xb_count,
        got, got2, ocn, ocn2, sea, area, w_atm, w_ocn,
        out, ocn_keep, ocn_send,
        tab_a, tab_o, num_a, num_o, trm_a, trm_o, acc_a, acc_o,
    ):
        t, s = pos[0], pos[1]
        per = got.shape[0]
        half = ocn.shape[1] // blk
        list_len = tab_a.shape[0]
        tab_a[:, f_a:, :] = jnp.ones((list_len, tab_a.shape[1] - f_a, blk), jnp.float32)
        tab_o[:, f_o:, :] = jnp.ones((2 * half, tab_o.shape[1] - f_o, blk), jnp.float32)
        for j in range(per):
            tab_a[s * per + j, :f_a] = got[j].astype(jnp.float32)
            tab_a[(1 - s) * per + j, :f_a] = got2[j].astype(jnp.float32)
        for j in range(half):
            at = slice(j * blk, (j + 1) * blk)
            tab_o[s * half + j, :f_o] = ocn[:, at].astype(jnp.float32)
            tab_o[(1 - s) * half + j, :f_o] = ocn2[:, at].astype(jnp.float32)
        xdims = (((1,), (1,)), ((), ()))
        for b in range(nblocks):
            num_a[b] = lax.dot_general(
                tab_a[xb_need[b]].astype(jnp.bfloat16), w_atm[b], xdims,
                preferred_element_type=jnp.float32,
            )
            num_o[b] = lax.dot_general(
                tab_o[xb_ocn[b]].astype(jnp.bfloat16), w_ocn[b], xdims,
                preferred_element_type=jnp.float32,
            )
        den_a = 1.0 / num_a[:, f_a, :]
        den_o = 1.0 / num_o[:, f_o, :]
        ta, qa, ua, va, ps, sw, lw, pr = [num_a[:, f, :] * den_a for f in range(8)]
        sst, uo, vo, oa = [num_o[:, f, :] * den_o for f in range(4)]
        du = ua - uo
        dv = va - vo
        speed = jnp.sqrt(du * du + dv * dv + 1.0)
        fac = (0.3 + 0.1 * jnp.tanh(ps)) * speed
        sens = fac * (sst - ta)
        lat = fac * (0.5 * sst - qa)
        taux = fac * du
        tauy = fac * dv
        albedo = 0.06 + 0.1 * jax.nn.sigmoid(oa)
        heat = (1.0 - albedo) * sw + lw - 0.2 * sst - sens - lat
        fresh = pr - 0.5 * lat
        rows = lax.broadcasted_iota(jnp.int32, (nblocks, blk), 0)
        weighted = jnp.where(rows < xb_count[0], area[...], 0.0)
        wet = weighted * sea[...].astype(jnp.float32)
        trm_a[...] = jnp.zeros_like(trm_a)
        trm_o[...] = jnp.zeros_like(trm_o)
        for g, v in enumerate((sens, lat, taux, tauy)):
            trm_a[:, g, :] = v * wet
        trm_a[:, 4, :] = weighted
        for g, v in enumerate((heat, taux, tauy, fresh)):
            trm_o[:, g, :] = v * wet
        trm_o[:, 4, :] = wet
        acc_a[...] = jnp.zeros_like(acc_a)
        acc_o[...] = jnp.zeros_like(acc_o)
        for b in range(nblocks):
            ya = jnp.dot(split3(trm_a[b]), w_atm[b], preferred_element_type=jnp.float32)
            yo = jnp.dot(split3(trm_o[b]), w_ocn[b], preferred_element_type=jnp.float32)
            acc_a[xb_need[b]] += ya[:ROWS] + ya[ROWS : 2 * ROWS] + ya[2 * ROWS :]
            acc_o[xb_ocn[b]] += yo[:ROWS] + yo[ROWS : 2 * ROWS] + yo[2 * ROWS :]
        row = lax.broadcasted_iota(jnp.int32, (ROWS, blk), 0)
        for i in range(list_len // 2):
            if ntile == len(shifts):
                slot = (t + (shifts[i] + ntile)) % ntile
            else:
                slot = i
            for e in range(2):
                n = 2 * i + e
                mine = need[n % per] % owned
                other = need2[n % per] % owned
                local = jnp.where(s == n // per, mine, other)
                msg = jnp.where(row < 5, acc_a[n], local.astype(jnp.float32))
                for d in range(nsub):
                    out[slot * nsub + d, e * ROWS : (e + 1) * ROWS] = msg
        for j in range(half):
            ocn_keep[j] = acc_o[s * half + j]
            ocn_send[j] = acc_o[(1 - s) * half + j]

    return body


def final_kernel(owned, blk, half, nflux):
    def body(recv, keep, got, atm, ocn, acc):
        acc[...] = jnp.zeros_like(acc)

        def add(m, _):
            for e in range(2):
                v = recv[m, e * ROWS : (e + 1) * ROWS]
                at = jnp.broadcast_to(v[5:6], v.shape)
                for a in range(owned):
                    acc[a] += jnp.where(at == float(a), v, 0.0)
            return 0

        lax.fori_loop(0, recv.shape[0], add, 0)
        for a in range(owned):
            v = acc[a]
            atm[:, a * blk : (a + 1) * blk] = v[:nflux] / jnp.maximum(v[nflux : nflux + 1], 1.0)
        for j in range(half):
            v = keep[j] + got[j]
            ocn[:, j * blk : (j + 1) * blk] = v[:nflux] / jnp.maximum(v[nflux : nflux + 1], 1.0)

    return body


def per_device(
    atm_state, ocn_state, need_atm, xb_need, xb_ocn, xb_count, sea_mask, cell_area, w_atm, w_ocn
):
    ntile = lax.axis_size("tile")
    nsub = lax.axis_size("sub")
    assert nsub == 2
    f_a, f_o = atm_state.shape[0], ocn_state.shape[0]
    nblocks, blk = w_atm.shape[:2]
    owned = atm_state.shape[1] // blk
    half = ocn_state.shape[1] // blk
    per = need_atm.shape[0]
    list_len = nsub * per
    pairs = list_len // 2
    shifts = [i - pairs // 2 + 1 if i < pairs - 1 else ntile // 2 for i in range(pairs)]
    here = per // 2
    t = lax.axis_index("tile")
    s = lax.axis_index("sub")
    pos = jnp.stack([t, s]).astype(jnp.int32)
    both = ("tile", "sub")

    def swap(x):
        return lax.ppermute(x, "sub", [(0, 1), (1, 0)])

    ocn2 = swap(ocn_state)
    need2 = swap(need_atm)
    states = []
    for j in range(here):
        route = []
        for d in range(nsub):
            k = shifts[d * here + j]
            if k:
                route += [(((u + k) % ntile) * nsub + d, u * nsub + d) for u in range(ntile)]
        states.append(lax.ppermute(atm_state, both, route))
    got = pl.pallas_call(
        select_kernel(here, owned, blk),
        out_shape=jax.ShapeDtypeStruct((per, f_a, blk), atm_state.dtype),
        in_specs=[SM, SM] + [VM] * (here + 1),
        out_specs=VM,
        name="select",
    )(pos, need_atm, *states[:-1], atm_state, states[-1])
    got2 = swap(got)
    f32 = jnp.float32
    out, keep, send = pl.pallas_call(
        main_kernel(nblocks, owned, blk, f_a, f_o, shifts, ntile, nsub),
        out_shape=(
            jax.ShapeDtypeStruct((pairs * nsub, 2 * ROWS, blk), f32),
            jax.ShapeDtypeStruct((half, ROWS, blk), f32),
            jax.ShapeDtypeStruct((half, ROWS, blk), f32),
        ),
        in_specs=[SM] * 6 + [VM] * 8,
        out_specs=(VM, VM, VM),
        scratch_shapes=[
            pltpu.VMEM((list_len, 16, blk), f32),
            pltpu.VMEM((nsub * half, 8, blk), f32),
            pltpu.VMEM((nblocks, 16, blk), f32),
            pltpu.VMEM((nblocks, 8, blk), f32),
            pltpu.VMEM((nblocks, ROWS, blk), f32),
            pltpu.VMEM((nblocks, ROWS, blk), f32),
            pltpu.VMEM((list_len, ROWS, blk), f32),
            pltpu.VMEM((nsub * half, ROWS, blk), f32),
        ],
        name="couple",
    )(
        pos, need_atm, need2, xb_need, xb_ocn, xb_count, got, got2, ocn_state, ocn2,
        sea_mask.reshape(nblocks, blk), cell_area.reshape(nblocks, blk), w_atm, w_ocn,
    )
    ocean = swap(send)
    if ntile == pairs:
        recv = lax.all_to_all(out, both, 0, 0, tiled=True)
    else:
        parts = []
        for i in range(pairs):
            k = shifts[i]
            for d in range(nsub):
                route = [
                    (u * nsub + c, ((u + k) % ntile) * nsub + (c + d) % nsub)
                    for u in range(ntile)
                    for c in range(nsub)
                ]
                parts.append(lax.ppermute(out[i * nsub + d], both, route))
        recv = jnp.stack(parts)
    nflux = 4
    return tuple(
        pl.pallas_call(
            final_kernel(owned, blk, half, nflux),
            out_shape=(
                jax.ShapeDtypeStruct((nflux, owned * blk), f32),
                jax.ShapeDtypeStruct((nflux, half * blk), f32),
            ),
            in_specs=[VM] * 3,
            out_specs=(VM, VM),
            scratch_shapes=[pltpu.VMEM((owned, ROWS, blk), f32)],
            name="finish",
        )(recv, keep, ocean)
    )


def solution(mesh):
    placed = (
        P(None, ("member", "tile")),
        P(None, ("member", "tile", "sub")),
        P(("tile", "sub")),
        P(("tile", "sub")),
        P(("tile", "sub")),
        P(("tile", "sub")),
        P(("tile", "sub")),
        P(("tile", "sub")),
        P(("tile", "sub"), None, None),
        P(("tile", "sub"), None, None),
    )
    return jax.shard_map(
        per_device,
        mesh=mesh,
        in_specs=placed,
        out_specs=(P(None, ("member", "tile")), P(None, ("member", "tile", "sub"))),
        check_vma=False,
    )
```

```python
import jax
import jax.numpy as jnp
from jax import lax
from jax.experimental import pallas as pl
from jax.experimental.pallas import tpu as pltpu
from jax.sharding import PartitionSpec as P

ROWS = 8
VM = pl.BlockSpec(memory_space=pltpu.VMEM)
SM = pl.BlockSpec(memory_space=pltpu.SMEM)


def split3(x):
    hi = x.astype(jnp.bfloat16)
    rest = x - hi.astype(jnp.float32)
    mid = rest.astype(jnp.bfloat16)
    lo = (rest - mid.astype(jnp.float32)).astype(jnp.bfloat16)
    return jnp.concatenate([hi, mid, lo], 0)


def before_kernel(nblocks, owned, blk, f_o):
    def body(need, need2, xb_ocn, ocn, ocn2, w_atm, w_ocn, fld_o, inv_a, loc, tab_o, num):
        s = lax.axis_index("sub")
        per = need.shape[0]
        half = ocn.shape[1] // blk
        tab_o[:, f_o:, :] = jnp.ones((2 * half, tab_o.shape[1] - f_o, blk), jnp.float32)
        for j in range(half):
            at = slice(j * blk, (j + 1) * blk)
            tab_o[s * half + j, :f_o] = ocn[:, at].astype(jnp.float32)
            tab_o[(1 - s) * half + j, :f_o] = ocn2[:, at].astype(jnp.float32)
        xdims = (((1,), (1,)), ((), ()))
        ones = jnp.ones((8, blk), jnp.bfloat16)
        for b in range(nblocks):
            num[b] = lax.dot_general(
                tab_o[xb_ocn[b]].astype(jnp.bfloat16), w_ocn[b], xdims,
                preferred_element_type=jnp.float32,
            )
            den = lax.dot_general(ones, w_atm[b], xdims, preferred_element_type=jnp.float32)
            inv_a[b : b + 1, :] = 1.0 / den[:1]
        inv_o = 1.0 / num[:, f_o, :]
        for f in range(f_o):
            fld_o[f] = num[:, f, :] * inv_o
        for n in range(2 * per):
            local = jnp.where(s == n // per, need[n % per], need2[n % per]) % owned
            loc[n] = jnp.broadcast_to((local * ROWS).astype(jnp.float32), (ROWS, blk))

    return body


def select_kernel(npair, owned, blk):
    def body(need, *refs):
        states, last, home, out = refs[: npair - 1], refs[npair - 1], refs[npair], refs[-1]
        s = lax.axis_index("sub")
        for j in range(npair):
            for e in range(2):
                n = need[2 * j + e] % owned
                at = pl.ds(pl.multiple_of(n * blk, blk), blk)
                if j < npair - 1:
                    out[2 * j + e] = states[j][:, at]
                else:
                    out[2 * j + e] = jnp.where(s == 0, home[:, at], last[:, at])

    return body


def main_kernel(nblocks, blk, shifts, ntile, nsub):
    def body(
        xb_need, xb_ocn, xb_count, got, got2, fld_o, inv_a, loc, sea, area, w_atm, w_ocn,
        out, ocn_keep, ocn_send,
        tab_a, num_a, trm_a, trm_o, acc_a, acc_o,
    ):
        t = lax.axis_index("tile")
        s = lax.axis_index("sub")
        per = got.shape[0]
        half = ocn_keep.shape[0]
        list_len = tab_a.shape[0]
        for j in range(per):
            tab_a[s * per + j] = got[j]
            tab_a[(1 - s) * per + j] = got2[j]
        xdims = (((1,), (1,)), ((), ()))
        for b in range(nblocks):
            num_a[b] = lax.dot_general(
                tab_a[xb_need[b]], w_atm[b], xdims, preferred_element_type=jnp.float32
            )
        ta, qa, ua, va, ps, sw, lw, pr = [num_a[:, f, :] * inv_a[...] for f in range(8)]
        sst, uo, vo, oa = [fld_o[f] for f in range(4)]
        du = ua - uo
        dv = va - vo
        speed = jnp.sqrt(du * du + dv * dv + 1.0)
        fac = (0.3 + 0.1 * jnp.tanh(ps)) * speed
        sens = fac * (sst - ta)
        lat = fac * (0.5 * sst - qa)
        taux = fac * du
        tauy = fac * dv
        albedo = 0.06 + 0.1 * jax.nn.sigmoid(oa)
        heat = (1.0 - albedo) * sw + lw - 0.2 * sst - sens - lat
        fresh = pr - 0.5 * lat
        rows = lax.broadcasted_iota(jnp.int32, (nblocks, blk), 0)
        weighted = jnp.where(rows < xb_count[0], area[...], 0.0)
        wet = weighted * sea[...].astype(jnp.float32)
        trm_a[...] = jnp.zeros_like(trm_a)
        trm_o[...] = jnp.zeros_like(trm_o)
        for g, v in enumerate((sens, lat, taux, tauy)):
            trm_a[:, g, :] = v * wet
        trm_a[:, 4, :] = weighted
        for g, v in enumerate((heat, taux, tauy, fresh)):
            trm_o[:, g, :] = v * wet
        trm_o[:, 4, :] = wet
        acc_a[...] = jnp.zeros_like(acc_a)
        acc_o[...] = jnp.zeros_like(acc_o)
        for b in range(nblocks):
            ya = jnp.dot(split3(trm_a[b]), w_atm[b], preferred_element_type=jnp.float32)
            yo = jnp.dot(split3(trm_o[b]), w_ocn[b], preferred_element_type=jnp.float32)
            acc_a[xb_need[b]] += ya[:ROWS] + ya[ROWS : 2 * ROWS] + ya[2 * ROWS :]
            acc_o[xb_ocn[b]] += yo[:ROWS] + yo[ROWS : 2 * ROWS] + yo[2 * ROWS :]
        row = lax.broadcasted_iota(jnp.int32, (ROWS, blk), 0)
        for i in range(list_len // 2):
            if ntile == len(shifts):
                slot = (t + (shifts[i] + ntile)) % ntile
            else:
                slot = i
            for e in range(2):
                msg = jnp.where(row < 5, acc_a[2 * i + e], loc[2 * i + e])
                for d in range(nsub):
                    out[slot * nsub + d, e * ROWS : (e + 1) * ROWS] = msg
        for j in range(half):
            ocn_keep[j] = acc_o[s * half + j]
            ocn_send[j] = acc_o[(1 - s) * half + j]

    return body


def final_kernel(owned, blk, half, nflux):
    def body(recv, keep, got, atm, ocn):
        total = recv.shape[0] * 2 * ROWS
        v = recv[...].reshape(total // ROWS, ROWS, blk)
        at = jnp.broadcast_to(v[:, 5:6, :], v.shape)
        key = at + lax.broadcasted_iota(jnp.int32, v.shape, 1).astype(jnp.float32)
        key = key.reshape(total, blk)
        v = v.reshape(total, blk)
        hi = v.astype(jnp.bfloat16)
        rest = v - hi.astype(jnp.float32)
        mid = rest.astype(jnp.bfloat16)
        lo = (rest - mid.astype(jnp.float32)).astype(jnp.bfloat16)
        parts = jnp.concatenate([hi, mid, lo], 1)
        lane = lax.broadcasted_iota(jnp.int32, (total, blk), 1).astype(jnp.float32)
        for c in range(-(-owned * ROWS // blk)):
            onehot = jnp.where(key == lane + float(c * blk), 1.0, 0.0).astype(jnp.bfloat16)
            y = lax.dot_general(
                onehot, parts, (((0,), (0,)), ((), ())), preferred_element_type=jnp.float32
            )
            y = y[:, :blk] + y[:, blk : 2 * blk] + y[:, 2 * blk :]
            for k in range(min(blk // ROWS, owned - c * (blk // ROWS))):
                a = c * (blk // ROWS) + k
                z = y[k * ROWS : (k + 1) * ROWS]
                atm[:, a * blk : (a + 1) * blk] = z[:nflux] / jnp.maximum(
                    z[nflux : nflux + 1], 1.0
                )
        for j in range(half):
            z = keep[j] + got[j]
            ocn[:, j * blk : (j + 1) * blk] = z[:nflux] / jnp.maximum(z[nflux : nflux + 1], 1.0)

    return body


def vmem(*xs):
    return [pltpu.with_memory_space_constraint(x, pltpu.VMEM) for x in xs]


def smem(*xs):
    return [pltpu.with_memory_space_constraint(x, pltpu.SMEM) for x in xs]


def per_device(
    atm_state, ocn_state, need_atm, xb_need, xb_ocn, xb_count, sea_mask, cell_area, w_atm, w_ocn
):
    ntile = lax.axis_size("tile")
    nsub = lax.axis_size("sub")
    assert nsub == 2
    f_a, f_o = atm_state.shape[0], ocn_state.shape[0]
    nblocks, blk = w_atm.shape[:2]
    owned = atm_state.shape[1] // blk
    half = ocn_state.shape[1] // blk
    per = need_atm.shape[0]
    list_len = nsub * per
    pairs = list_len // 2
    shifts = [i - pairs // 2 + 1 if i < pairs - 1 else ntile // 2 for i in range(pairs)]
    here = per // 2
    both = ("tile", "sub")
    f32 = jnp.float32

    def swap(x):
        return lax.ppermute(x, "sub", [(0, 1), (1, 0)])

    ocn2 = swap(ocn_state)
    need2 = swap(need_atm)
    states = []
    for j in range(here):
        route = []
        for d in range(nsub):
            k = shifts[d * here + j]
            if k:
                route += [(((u + k) % ntile) * nsub + d, u * nsub + d) for u in range(ntile)]
        states.append(lax.ppermute(atm_state, both, route))
    wa, wo = vmem(w_atm, w_ocn)
    need_s, xn, xo, xc = smem(need_atm, xb_need, xb_ocn, xb_count)
    fld_o, inv_a, loc = pl.pallas_call(
        before_kernel(nblocks, owned, blk, f_o),
        out_shape=(
            pltpu.VMEM((f_o, nblocks, blk), f32),
            pltpu.VMEM((nblocks, blk), f32),
            pltpu.VMEM((list_len, ROWS, blk), f32),
        ),
        in_specs=[SM] * 3 + [VM] * 4,
        out_specs=(VM, VM, VM),
        scratch_shapes=[
            pltpu.VMEM((nsub * half, 8, blk), f32),
            pltpu.VMEM((nblocks, 8, blk), f32),
        ],
        name="before",
    )(need_s, *smem(need2), xo, *vmem(ocn_state, ocn2), wa, wo)
    got = pl.pallas_call(
        select_kernel(here, owned, blk),
        out_shape=pltpu.VMEM((per, f_a, blk), atm_state.dtype),
        in_specs=[SM] + [VM] * (here + 2),
        out_specs=VM,
        name="select",
    )(need_s, *vmem(*states, atm_state, inv_a))
    got2 = swap(got)
    out, keep, send = pl.pallas_call(
        main_kernel(nblocks, blk, shifts, ntile, nsub),
        out_shape=(
            pltpu.VMEM((pairs * nsub, 2 * ROWS, blk), f32),
            pltpu.VMEM((half, ROWS, blk), f32),
            pltpu.VMEM((half, ROWS, blk), f32),
        ),
        in_specs=[SM] * 3 + [VM] * 9,
        out_specs=(VM, VM, VM),
        scratch_shapes=[
            pltpu.VMEM((list_len, f_a, blk), atm_state.dtype),
            pltpu.VMEM((nblocks, 8, blk), f32),
            pltpu.VMEM((nblocks, ROWS, blk), f32),
            pltpu.VMEM((nblocks, ROWS, blk), f32),
            pltpu.VMEM((list_len, ROWS, blk), f32),
            pltpu.VMEM((nsub * half, ROWS, blk), f32),
        ],
        name="couple",
    )(
        xn, xo, xc, *vmem(got, got2, fld_o, inv_a, loc),
        *vmem(sea_mask.reshape(nblocks, blk), cell_area.reshape(nblocks, blk)), wa, wo,
    )
    ocean = swap(send)
    if ntile == pairs:
        recv = lax.all_to_all(out, both, 0, 0, tiled=True)
    else:
        parts = []
        for i in range(pairs):
            k = shifts[i]
            for d in range(nsub):
                route = [
                    (u * nsub + c, ((u + k) % ntile) * nsub + (c + d) % nsub)
                    for u in range(ntile)
                    for c in range(nsub)
                ]
                parts.append(lax.ppermute(out[i * nsub + d], both, route))
        recv = jnp.stack(parts)
    nflux = 4
    return tuple(
        pl.pallas_call(
            final_kernel(owned, blk, half, nflux),
            out_shape=(
                jax.ShapeDtypeStruct((nflux, owned * blk), f32),
                jax.ShapeDtypeStruct((nflux, half * blk), f32),
            ),
            in_specs=[VM] * 3,
            out_specs=(VM, VM),
            name="finish",
        )(*vmem(recv, keep, ocean))
    )


def solution(mesh):
    placed = (
        P(None, ("member", "tile")),
        P(None, ("member", "tile", "sub")),
        P(("tile", "sub")),
        P(("tile", "sub")),
        P(("tile", "sub")),
        P(("tile", "sub")),
        P(("tile", "sub")),
        P(("tile", "sub")),
        P(("tile", "sub"), None, None),
        P(("tile", "sub"), None, None),
    )
    return jax.shard_map(
        per_device,
        mesh=mesh,
        in_specs=placed,
        out_specs=(P(None, ("member", "tile")), P(None, ("member", "tile", "sub"))),
        check_vma=False,
    )
```
